32 devices in a mesh: pipe: 4 (over x, core), vocab: 8 (over z, y).
Axes of the slice: x: 2, y: 2, z: 4, core: 2. Of those that a mesh axis runs over, the one named last changes fastest.
Arguments:
- hidden: bfloat16 [4, 128, 4096], P('pipe'), may hold values from -60 to 60
- norm_gain: float32 [4096], replicated, may hold values from 0.5 to 1.5
- out_weight: bfloat16 [128256, 4096], P(('pipe', 'vocab')), may hold values from -4 to 4
- targets: int32 [4, 128], P('pipe'), may hold values from 0 to 128255
- loss_mask: int32 [4, 128], P('pipe'), may hold values from 0 to 1, as said below
- slot_position: int32 [4, 128], P('pipe'), may hold values from 0 to 127, each once within a row
- counts: int32 [4], replicated, may hold values from 1 to 128, 320 in all
- loss_scale: float32 [], replicated, may hold values from 4096 to 32768
Outputs:
- loss: float32 [], replicated
- grad_hidden: bfloat16 [4, 128, 4096], P('pipe')
The draws below stay inside these ranges and needn't reach their ends.
Inputs may be any that keep to these rules, and one draw needn't show every extreme that they name: The 4 counts sum to exactly 320, and one of them equals 128. Each row of slot_position holds every number of 0 to 127 once. Each row of loss_mask holds at least 64 ones.
All inputs are finite; a program needn't handle non-finite values.
Results may differ from the reference program's by a relative error of at most 0.0034.
Values may be sent and summed in bfloat16 or wider, within the bound.
A program may use at most 128 MiB of HBM per device.

```python
import math
import jax
import jax.numpy as jnp
import numpy as np
from jax import lax

D = 4096
VOCAB = 128256
TOK_MB = 128
MICRO = 4
LIVE = 320


def make_hidden(key):
    folded = jax.random.fold_in(key, 11)
    key_scale, key_noise = jax.random.split(folded)
    scales = jnp.exp(jax.random.uniform(key_scale, (MICRO, TOK_MB, 1), jnp.float32) * math.log(10.0))
    raw_noise = jnp.clip(jax.random.normal(key_noise, (MICRO, TOK_MB, D), jnp.float32), -6.0, 6.0)
    return raw_noise * scales


def draw_hidden(key, part):
    return make_hidden(key).astype(jnp.bfloat16)


def draw_out_weight(key, part):
    folded = jax.random.fold_in(key, 23)
    key_weight = jax.random.fold_in(folded, 0)
    weight = jnp.clip(jax.random.normal(key_weight, (VOCAB, D), jnp.float32), -6.0, 6.0) * (3.0 / math.sqrt(D))
    return weight.astype(jnp.bfloat16)


def draw_loss_mask(key, part):
    folded = jax.random.fold_in(key, 37)
    key_count, key_order = jax.random.split(folded)
    ones_count = jax.random.randint(key_count, (MICRO, 1), TOK_MB // 2, TOK_MB + 1)
    order_keys = jax.random.split(key_order, MICRO)
    ranks = jax.vmap(lambda one_key: jax.random.permutation(one_key, TOK_MB))(order_keys)
    return jnp.where(ranks < ones_count, 1, 0).astype(jnp.int32)


def place_ends(entries, rng, low, largest):
    longest = entries.shape.index(max(entries.shape))
    spots = []
    for shift in (0, 1):
        where = [jax.random.randint(jax.random.fold_in(rng, axis), (), 0, length) for axis, length in enumerate(entries.shape)]
        where[longest] = (where[longest] + shift) % entries.shape[longest]
        spots.append(tuple(where))
    return entries.at[spots[0]].set(low).at[spots[1]].set(largest)


def ranked_wide(own_key, shape, count, lean):
    weights = [min(1 << octave, count + 1 - (1 << octave)) * (1 << 20) // math.isqrt((1 << octave) ** lean) + 1 for octave in range((count + 1).bit_length()) if 1 << octave <= count]
    spread = 1 + sum(weights) // (1 << 30)
    table = np.cumsum(np.array([max(1, weight // spread) for weight in weights]))
    lot = jax.random.randint(jax.random.fold_in(own_key, 1), shape, 0, int(table[len(weights) - 1]))
    start = jnp.left_shift(1, jnp.searchsorted(jnp.asarray(table, jnp.int32), lot, side="right").astype(jnp.int32))
    standing = start - 1 + jax.random.randint(jax.random.fold_in(own_key, 4), shape, 0, 1 << 30) % jnp.minimum(start, count + 1 - start)
    return jax.random.permutation(jax.random.fold_in(own_key, 2), count)[standing].astype(jnp.int32)


def length_profile(amount, total, bound, skew):
    weights = [(1 << 20) // math.isqrt(rank ** skew) + 1 for rank in range(2, amount + 1)]
    spare, holding = total - bound - (amount - 1), [1] * (amount - 1)
    while spare > 0:
        movable = [i for i in range(amount - 1) if holding[i] < bound]
        whole, left = sum([weights[i] for i in movable]), spare
        for i in movable:
            addition = min(bound - holding[i], max(1, left * weights[i] // whole), spare)
            holding[i] = holding[i] + addition
            spare = spare - addition
    return np.array([bound] + holding)


def uneven_parts(own_key, number_of, total, reach, lean):
    if number_of == 2:
        one = jax.random.randint(own_key, (), max(1, total - reach), min(reach, total - 1) + 1)
        return jnp.stack([one, total - one])
    sizes = jnp.asarray(length_profile(number_of, total, reach, lean), jnp.int32)
    couples = (number_of - 1) // 2
    donor, sink = sizes[1:1 + 2 * couples:2], sizes[2:2 + 2 * couples:2]
    margin = jnp.minimum(donor - 1, reach - sink)
    shifted = jax.random.randint(jax.random.fold_in(own_key, 1), (couples,), 0, 1 << 20) % (margin + 1)
    sizes = sizes.at[1:1 + 2 * couples:2].set(donor - shifted).at[2:2 + 2 * couples:2].set(sink + shifted)
    return sizes[jax.random.permutation(jax.random.fold_in(own_key, 2), number_of)]


def setup_inputs(seed: int = 0) -> dict:
    seeds = jax.random.split(jax.random.key(seed), 9)
    return {
        "hidden": draw_hidden(jax.random.fold_in(seeds[8], 71), 0),
        "norm_gain": jnp.clip(1.0 + 0.1 * jax.random.normal(seeds[1], (D,), jnp.float32), 0.5, 1.5),
        "out_weight": draw_out_weight(jax.random.fold_in(seeds[8], 71), 0),
        "targets": place_ends(ranked_wide(seeds[3], (MICRO, TOK_MB), VOCAB, 2), jax.random.fold_in(seeds[3], 3), 0, VOCAB - 1).astype(jnp.int32),
        "loss_mask": draw_loss_mask(jax.random.fold_in(seeds[8], 71), 0),
        "slot_position": jax.vmap(lambda own: jax.random.permutation(own, TOK_MB))(jax.random.split(seeds[5], MICRO)).reshape((MICRO, TOK_MB)).astype(jnp.int32),
        "counts": uneven_parts(seeds[6], MICRO, LIVE, TOK_MB, 2).astype(jnp.int32),
        "loss_scale": jnp.clip(jnp.exp(jax.random.uniform(seeds[7], (), jnp.float32, math.log(4096.0), math.log(32768.0))), 4096.0, 32768.0),
    }


EPSILON = 1e-05

def rms_scale(values, norm_gain):
    mean_square = lax.optimization_barrier(jnp.mean(values * values, axis=-1, keepdims=True))
    return values * lax.rsqrt(mean_square + EPSILON) * norm_gain.astype(jnp.float32)

def micro_terms(normed_rows, target_row, weight_row, out_weight, loss_scale, weight_total):
    logits = lax.dot_general(normed_rows, out_weight, (((1,), (1,)), ((), ())), preferred_element_type=jnp.float32)
    row_top = lax.optimization_barrier(jnp.max(logits, axis=1))
    exp_total = lax.optimization_barrier(jnp.sum(jnp.exp(logits - row_top[:, None]), axis=1))
    log_total = row_top + jnp.log(exp_total)
    is_target = jnp.arange(VOCAB, dtype=jnp.int32)[None, :] == target_row.astype(jnp.int32)[:, None]
    target_logit = lax.optimization_barrier(jnp.sum(jnp.where(is_target, logits, 0.0), axis=1))
    loss_part = jnp.sum(weight_row * (log_total - target_logit))
    token_coef = loss_scale * weight_row / weight_total
    logit_grad = ((jnp.exp(logits - log_total[:, None]) - is_target.astype(jnp.float32)) * token_coef[:, None]).astype(jnp.bfloat16)
    normed_grad = jnp.dot(logit_grad, out_weight, preferred_element_type=jnp.float32)
    return (loss_part, normed_grad)

def reference(hidden, norm_gain, out_weight, targets, loss_mask, slot_position, counts, loss_scale):
    rows_total = MICRO * TOK_MB
    flat = hidden.reshape(rows_total, D).astype(jnp.float32)
    normed = rms_scale(flat, norm_gain).astype(jnp.bfloat16)
    inside = slot_position < counts[:, None]
    token_weight = jnp.where(inside & (loss_mask == 1), 1.0, 0.0).astype(jnp.float32)
    weight_total = jnp.sum(token_weight)

    def one_micro(item):
        return micro_terms(item[0], item[1], item[2], out_weight, loss_scale, weight_total)
    loss_parts, normed_grad = lax.map(one_micro, (normed.reshape(MICRO, TOK_MB, D), targets, token_weight))
    loss = jnp.sum(loss_parts) / weight_total
    pullback = jax.vjp(lambda values: rms_scale(values, norm_gain), flat)[1]
    grad_flat = pullback(normed_grad.reshape(rows_total, D))[0]
    return (loss, grad_flat.astype(jnp.bfloat16).reshape(MICRO, TOK_MB, D))
```

```python
import functools
import jax
import jax.numpy as jnp
from jax import lax
from jax.experimental import pallas as pl
from jax.experimental.pallas import tpu as pltpu
from jax.sharding import PartitionSpec as P

EPSILON = 1e-05
MESH = pl.DeviceIdType.MESH
F32 = jnp.float32
BF16 = jnp.bfloat16
VMEM = pl.BlockSpec(memory_space=pltpu.VMEM)


def rms_scale(values, norm_gain):
    mean_square = jnp.mean(values * values, axis=-1, keepdims=True)
    return values * lax.rsqrt(mean_square + EPSILON) * norm_gain


def pull_rows(rows, norm_gain, cotangent):
    pullback = jax.vjp(lambda values: rms_scale(values, norm_gain), rows)[1]
    return pullback(cotangent)[0].astype(BF16)


def place(ny):
    p, v = lax.axis_index("pipe"), lax.axis_index("vocab")
    return p // 2, p % 2, v % ny, v // ny


def greet(targets):
    barrier = pltpu.get_barrier_semaphore()
    for target in targets:
        pl.semaphore_signal(barrier, inc=1, device_id=target, device_id_type=MESH)
    pl.semaphore_wait(barrier, len(targets))


def remote(src, dst, send, recv, target):
    return pltpu.make_async_remote_copy(
        src_ref=src, dst_ref=dst, send_sem=send, recv_sem=recv,
        device_id=target, device_id_type=MESH,
    )


def gather_kernel(ny, chunks, own, ints, out, oints, sems_s, sems_r, own_s, own_r, int_s, int_r):
    x, core, y, z = place(ny)
    p, v = x * 2 + core, z * ny + y
    mate = (x * 2 + (1 - core), v)
    across = ((1 - x) * 2 + core, v)
    diag = ((1 - x) * 2 + (1 - core), v)
    beside = (p, z * ny + (1 - y))
    greet([mate, across, diag, beside])
    far = (1 - x) * 2 + core
    started = []
    first = []
    for c in range(chunks):
        cp = remote(own.at[y, c], out.at[p, y, c], sems_s.at[0, c], sems_r.at[0, c], across)
        cp.start()
        first.append(cp)
    for j, target in enumerate((mate, across, diag)):
        cp = remote(ints, oints.at[p], int_s.at[j], int_r.at[j], target)
        cp.start()
        started.append(cp)
    cp = remote(own, out.at[p], own_s, own_r, mate)
    cp.start()
    started.append(cp)
    oints[p] = ints[...]
    out[p] = own[...]
    second = []
    for c in range(chunks):
        first[c].wait_recv()
        cy = remote(out.at[far, y, c], out.at[far, y, c], sems_s.at[1, c], sems_r.at[1, c], beside)
        cy.start()
        cm = remote(out.at[far, y, c], out.at[far, y, c], sems_s.at[2, c], sems_r.at[2, c], mate)
        cm.start()
        second.append(cy)
        started.append(cm)
    for c in range(chunks):
        second[c].wait_recv()
        cm = remote(out.at[far, 1 - y, c], out.at[far, 1 - y, c], sems_s.at[3, c], sems_r.at[3, c], mate)
        cm.start()
        started.append(cm)
    for cp in started:
        cp.wait_recv()
    for cp in first + second + started:
        cp.wait_send()


def gather(own, ints, pipe, ny, chunks):
    rows, width = own.shape
    part = rows // (2 * chunks)
    out, oints = pl.pallas_call(
        functools.partial(gather_kernel, ny, chunks),
        out_shape=(
            jax.ShapeDtypeStruct((pipe, 2, chunks, part, width), BF16),
            jax.ShapeDtypeStruct((pipe,) + ints.shape, jnp.int32),
        ),
        in_specs=[VMEM, VMEM],
        out_specs=(VMEM, VMEM),
        scratch_shapes=[
            pltpu.SemaphoreType.DMA((4, chunks)),
            pltpu.SemaphoreType.DMA((4, chunks)),
            pltpu.SemaphoreType.DMA,
            pltpu.SemaphoreType.DMA,
            pltpu.SemaphoreType.DMA((3,)),
            pltpu.SemaphoreType.DMA((3,)),
        ],
        compiler_params=pltpu.CompilerParams(
            collective_id=0, has_side_effects=True, vmem_limit_bytes=24 * 2**20
        ),
    )(own.reshape(2, chunks, part, width), ints)
    return out.reshape(pipe * rows, width), oints


def stats_kernel(pipe, vocab, st, out, box, send, recv):
    p, v = lax.axis_index("pipe"), lax.axis_index("vocab")
    peers = []
    for dp in range(pipe):
        for dv in range(vocab):
            if dp or dv:
                peers.append((lax.rem(p + dp, pipe), lax.rem(v + dv, vocab)))
    greet(peers)
    copies = []
    for j, target in enumerate(peers):
        cp = remote(st, box.at[j], send.at[j], recv.at[j], target)
        cp.start()
        copies.append(cp)
    for cp in copies:
        cp.wait_recv()
    n = st.shape[1]
    own_top = st[0]
    tops = box[:, 0]
    top = jnp.maximum(own_top, jnp.max(tops, axis=0))
    total = st[1] * jnp.exp(own_top - top) + jnp.sum(
        box[:, 1] * jnp.exp(tops - top[None]), axis=0
    )
    out[0] = top + jnp.log(total)
    out[1] = st[2] + jnp.sum(box[:, 2], axis=0)
    for cp in copies:
        cp.wait_send()


def combine_stats(top, total, target, pipe, vocab):
    rows = top.shape[0]
    st = jnp.stack([top, total, target]).reshape(3, rows // 128, 128)
    n = pipe * vocab - 1
    out = pl.pallas_call(
        functools.partial(stats_kernel, pipe, vocab),
        out_shape=jax.ShapeDtypeStruct((2, rows // 128, 128), F32),
        in_specs=[VMEM],
        out_specs=VMEM,
        scratch_shapes=[
            pltpu.VMEM((n,) + st.shape, F32),
            pltpu.SemaphoreType.DMA((n,)),
            pltpu.SemaphoreType.DMA((n,)),
        ],
        compiler_params=pltpu.CompilerParams(collective_id=1, has_side_effects=True),
    )(st)
    return out[0].reshape(rows), out[1].reshape(rows)


def reduce_kernel(ny, nz, g, h, gain, out, ra, sb1, sb2, rb1, rb2, sc1, sc2, rc1, rc2,
                  u, sd, rd, s_a, r_a, s_b, r_b, s_c, r_c, s_d, r_d, s_e, r_e, s_f, r_f):
    x, core, y, z = place(ny)
    p, v = x * 2 + core, z * ny + y
    half = g.shape[-1] // 2
    lo, hi = pl.ds(0, half), pl.ds(half, half)
    mate = (x * 2 + (1 - core), v)
    across = ((1 - x) * 2 + core, v)
    beside = (p, z * ny + (1 - y))
    along = [(p, lax.rem(z + d, nz) * ny + y) for d in range(1, nz)]
    greet([mate, across, beside] + along)
    copies = []

    def go(src, dst, send, recv, target):
        cp = remote(src, dst, send, recv, target)
        cp.start()
        copies.append(cp)
        return cp

    order = ((1 - x, 1 - y), (1 - x, y), (x, 1 - y), (x, y))
    pa = [go(g.at[a, 1 - core, b], ra.at[a, b], s_a.at[j], r_a.at[j], mate)
          for j, (a, b) in enumerate(order)]

    def fill(dst, i, a, b, cols):
        def one(k, carry):
            dst[i, k] = (g[a, core, b, k, :, cols] + ra[a, b, k, :, cols]).astype(BF16)
            return carry
        lax.fori_loop(0, nz, one, 0)

    pa[0].wait_recv()
    fill(sb1, 1 - y, 1 - x, 1 - y, lo)
    b10 = go(sb1.at[1 - y], rb1.at[1 - y], s_b.at[0], r_b.at[0], across)
    fill(sb2, 1 - x, 1 - x, 1 - y, hi)
    b20 = go(sb2.at[1 - x], rb2.at[1 - x], s_b.at[1], r_b.at[1], beside)
    pa[1].wait_recv()
    fill(sb1, y, 1 - x, y, lo)
    b11 = go(sb1.at[y], rb1.at[y], s_b.at[2], r_b.at[2], across)
    pa[2].wait_recv()
    fill(sb2, x, x, 1 - y, hi)
    b21 = go(sb2.at[x], rb2.at[x], s_b.at[3], r_b.at[3], beside)
    pa[3].wait_recv()

    b10.wait_recv()

    def fc1(k, carry):
        sc1[k] = (g[x, core, 1 - y, k, :, lo] + ra[x, 1 - y, k, :, lo]
                  + rb1[1 - y, k].astype(F32)).astype(BF16)
        return carry
    lax.fori_loop(0, nz, fc1, 0)
    b20.wait_recv()

    def fc2(k, carry):
        sc2[k] = (g[1 - x, core, y, k, :, hi] + ra[1 - x, y, k, :, hi]
                  + rb2[1 - x, k].astype(F32)).astype(BF16)
        return carry
    lax.fori_loop(0, nz, fc2, 0)
    c1 = go(sc1, rc1, s_c.at[0], r_c.at[0], beside)
    c2 = go(sc2, rc2, s_c.at[1], r_c.at[1], across)
    b11.wait_recv()
    b21.wait_recv()
    c1.wait_recv()
    c2.wait_recv()

    def fu(k, carry):
        a = (g[x, core, y, k, :, lo] + ra[x, y, k, :, lo]
             + rb1[y, k].astype(F32) + rc1[k].astype(F32))
        b = (g[x, core, y, k, :, hi] + ra[x, y, k, :, hi]
             + rb2[x, k].astype(F32) + rc2[k].astype(F32))
        u[k, :, lo] = a
        u[k, :, hi] = b
        sd[k, :, lo] = a.astype(BF16)
        sd[k, :, hi] = b.astype(BF16)
        return carry
    lax.fori_loop(0, nz, fu, 0)
    pd = [go(sd.at[lax.rem(z + d, nz)], rd.at[d - 1], s_d.at[d - 1], r_d.at[d - 1], along[d - 1])
          for d in range(1, nz)]
    rows = h[y, z].astype(F32)
    scale = lax.rsqrt(jnp.mean(rows * rows, axis=-1, keepdims=True) + EPSILON)
    for cp in pd:
        cp.wait_recv()
    total = u[z]
    for d in range(1, nz):
        total = total + rd[d - 1].astype(F32)
    gg = total * gain[...]
    dot = jnp.mean(rows * gg, axis=-1, keepdims=True)
    out[y, z] = (scale * gg - (scale * scale * scale) * rows * dot).astype(BF16)

    tail = [go(out.at[y, z], out.at[y, z], s_f.at[0], r_f.at[0], beside)]
    pe = [go(out.at[y, z], out.at[y, z], s_e.at[d - 1], r_e.at[d - 1], along[d - 1])
          for d in range(1, nz)]
    for d in range(1, nz):
        pe[d - 1].wait_recv()
        zz = lax.rem(z + nz - d, nz)
        tail.append(go(out.at[y, zz], out.at[y, zz], s_f.at[d], r_f.at[d], beside))
    for cp in tail:
        cp.wait_recv()
    for cp in copies:
        cp.wait_send()


def reduce_finish(grad, rows, norm_gain, ny, nz):
    micro, width = rows.shape
    part = micro // (ny * nz)
    half = width // 2
    dma = pltpu.SemaphoreType.DMA
    out = pl.pallas_call(
        functools.partial(reduce_kernel, ny, nz),
        out_shape=jax.ShapeDtypeStruct((ny, nz, part, width), BF16),
        in_specs=[VMEM] * 3,
        out_specs=VMEM,
        scratch_shapes=[
            pltpu.VMEM((2, ny, nz, part, width), F32),
            pltpu.VMEM((ny, nz, part, half), BF16),
            pltpu.VMEM((2, nz, part, half), BF16),
            pltpu.VMEM((ny, nz, part, half), BF16),
            pltpu.VMEM((2, nz, part, half), BF16),
            pltpu.VMEM((nz, part, half), BF16),
            pltpu.VMEM((nz, part, half), BF16),
            pltpu.VMEM((nz, part, half), BF16),
            pltpu.VMEM((nz, part, half), BF16),
            pltpu.VMEM((nz, part, width), F32),
            pltpu.VMEM((nz, part, width), BF16),
            pltpu.VMEM((nz - 1, part, width), BF16),
            dma((4,)), dma((4,)), dma((4,)), dma((4,)), dma((2,)), dma((2,)),
            dma((nz - 1,)), dma((nz - 1,)), dma((nz - 1,)), dma((nz - 1,)), dma((nz,)), dma((nz,)),
        ],
        compiler_params=pltpu.CompilerParams(
            collective_id=2, has_side_effects=True, vmem_limit_bytes=40 * 2**20
        ),
    )(
        grad.reshape(2, 2, ny, nz, part, width),
        rows.reshape(ny, nz, part, width),
        norm_gain.reshape(1, width),
    )
    return out


def body(pipe, vocab, hidden, norm_gain, out_weight, targets, loss_mask, slot_position, counts, loss_scale):
    micro_slots = hidden.shape[1]
    model_width = hidden.shape[2]
    shard_words = out_weight.shape[0]
    ny = 2
    nz = vocab // ny
    fast = pipe == 4 and vocab == ny * nz and nz <= 4 and micro_slots == 16 * vocab
    offset = lax.axis_index(("pipe", "vocab")) * shard_words
    own_rows = hidden.reshape(micro_slots, model_width).astype(F32)
    own_normed = rms_scale(own_rows, norm_gain).astype(BF16)
    own_ints = jnp.concatenate(
        [targets, loss_mask, slot_position, jnp.zeros((5, micro_slots), jnp.int32)], axis=0
    )
    if fast:
        all_normed, all_ints = gather(own_normed, own_ints, pipe, ny, 4)
    else:
        all_normed = lax.all_gather(own_normed, "pipe", axis=0, tiled=True)
        all_ints = lax.all_gather(own_ints, "pipe", axis=0)
    rows_total = all_normed.shape[0]
    all_targets, all_masks, all_positions = (
        all_ints[:, k].reshape(rows_total) for k in range(3)
    )
    count_row = jnp.broadcast_to(counts[:, None], (counts.shape[0], micro_slots)).reshape(rows_total)
    inside = all_positions < count_row
    token_weight = jnp.where(inside & (all_masks == 1), 1.0, 0.0).astype(F32)
    weight_total = jnp.sum(token_weight)
    logits = lax.dot_general(
        all_normed, out_weight, (((1,), (1,)), ((), ())), preferred_element_type=F32
    )
    is_target = (
        jnp.arange(shard_words, dtype=jnp.int32)[None, :] == (all_targets - offset)[:, None]
    )
    local_target = jnp.sum(jnp.where(is_target, logits, 0.0), axis=1)
    local_top = jnp.max(logits, axis=1)
    if fast:
        local_total = jnp.sum(jnp.exp(logits - local_top[:, None]), axis=1)
        log_total, target_logit = combine_stats(local_top, local_total, local_target, pipe, vocab)
    else:
        row_top = lax.pmax(local_top, ("pipe", "vocab"))
        local_total = jnp.sum(jnp.exp(logits - row_top[:, None]), axis=1)
        exp_total, target_logit = lax.psum((local_total, local_target), ("pipe", "vocab"))
        log_total = row_top + jnp.log(exp_total)
    loss = jnp.sum(token_weight * (log_total - target_logit)) / weight_total
    token_coef = loss_scale * token_weight / weight_total
    logit_grad = (
        (jnp.exp(logits - log_total[:, None]) - is_target.astype(F32)) * token_coef[:, None]
    ).astype(BF16)
    work_grad = jnp.dot(logit_grad, out_weight, preferred_element_type=F32)
    if fast:
        grad_out = reduce_finish(work_grad, hidden.reshape(micro_slots, model_width), norm_gain, ny, nz)
    else:
        grad_cube = work_grad.reshape(rows_total // micro_slots, micro_slots, model_width)
        micro_grad = lax.psum_scatter(grad_cube, "pipe", scatter_dimension=0, tiled=True)
        summed = lax.psum(micro_grad, "vocab")
        grad_out = pull_rows(own_rows, norm_gain, summed.reshape(micro_slots, model_width))
    return (loss, grad_out.reshape(1, micro_slots, model_width))


def solution(mesh):
    in_specs = (
        P("pipe", None, None),
        P(),
        P(("pipe", "vocab"), None),
        P("pipe", None),
        P("pipe", None),
        P("pipe", None),
        P(),
        P(),
    )
    out_specs = (P(), P("pipe", None, None))
    part = functools.partial(body, mesh.shape["pipe"], mesh.shape["vocab"])
    return jax.shard_map(part, mesh=mesh, in_specs=in_specs, out_specs=out_specs, check_vma=False)
```
